8 devices in a mesh: dp: 1 (over z), m1: 2 (over y), m2: 4 (over x, core).
Axes of the slice: x: 2, y: 2, z: 1, core: 2. Of those that a mesh axis runs over, the one named last changes fastest.
Arguments:
- x: bfloat16 [32, 256, 8192], P('dp', None, 'm1')
- ln_scale: float32 [8192], replicated
- qn_scale: float32 [128], replicated
- kn_scale: float32 [128], replicated
- w_qkv: bfloat16 [8192, 3, 8192], P('m1', None, 'm2')
- w_up: bfloat16 [8192, 22528], P('m1', 'm2')
- b_up: float32 [22528], P('m2')
- w_o: bfloat16 [8192, 8192], P('m2', 'm1')
- w_down: bfloat16 [22528, 8192], P('m2', 'm1')
- b_out: float32 [8192], P('m1')
Outputs:
- output: bfloat16 [32, 256, 8192], P('dp', None, 'm1')
All inputs are finite; a program needn't handle non-finite values.
Results may differ from the reference program's by a relative error of at most 0.00976899.
Values are sent between devices in bfloat16 or wider.
A program may use at most 1.25 GiB of HBM per device.

```python
import jax
import jax.numpy as jnp
from jax import lax

BATCH = 32
PATCHES = 256
MODEL_DIM = 8192
HEADS = 64
HEAD_DIM = 128
MLP_DIM = 22528
LN_EPS = 1e-6


def setup_inputs(seed: int = 0, part: int = 0) -> dict:
    part_key = jax.random.fold_in(jax.random.key(seed), part)
    key_mean, key_scale, key_noise = jax.random.split(part_key, 3)
    shared = jax.random.split(jax.random.key(seed + 1), 9)
    qkv_width = HEADS * HEAD_DIM
    tok_mean = 1.5 * jax.random.normal(key_mean, (BATCH, PATCHES, 1), jnp.float32)
    tok_scale = jax.random.uniform(key_scale, (BATCH, PATCHES, 1), jnp.float32, 0.5, 2.0)
    col_scale = 0.5 + 1.5 * jnp.arange(MODEL_DIM, dtype=jnp.float32) / MODEL_DIM
    noise = jax.random.normal(key_noise, (BATCH, PATCHES, MODEL_DIM), jnp.float32)
    x = (tok_mean + tok_scale * col_scale * noise).astype(jnp.bfloat16)
    ln_scale = jax.random.uniform(shared[0], (MODEL_DIM,), jnp.float32, 0.5, 1.5)
    qn_scale = jax.random.uniform(shared[1], (HEAD_DIM,), jnp.float32, 1.0, 2.5)
    kn_scale = jax.random.uniform(shared[2], (HEAD_DIM,), jnp.float32, 1.0, 2.5)
    w_qkv = (jax.random.normal(shared[3], (MODEL_DIM, 3, qkv_width), jnp.float32) * MODEL_DIM ** -0.5).astype(jnp.bfloat16)
    w_up = (jax.random.normal(shared[4], (MODEL_DIM, MLP_DIM), jnp.float32) * MODEL_DIM ** -0.5).astype(jnp.bfloat16)
    b_up = 0.5 * jax.random.normal(shared[5], (MLP_DIM,), jnp.float32)
    w_o = (jax.random.normal(shared[6], (qkv_width, MODEL_DIM), jnp.float32) * qkv_width ** -0.5).astype(jnp.bfloat16)
    w_down = (jax.random.normal(shared[7], (MLP_DIM, MODEL_DIM), jnp.float32) * MLP_DIM ** -0.5).astype(jnp.bfloat16)
    b_out = 0.5 * jax.random.normal(shared[8], (MODEL_DIM,), jnp.float32)
    return {'x': x, 'ln_scale': ln_scale, 'qn_scale': qn_scale, 'kn_scale': kn_scale, 'w_qkv': w_qkv, 'w_up': w_up, 'b_up': b_up, 'w_o': w_o, 'w_down': w_down, 'b_out': b_out}


def layer_norm(values, scale):
    mean = jnp.mean(values, axis=-1, keepdims=True)
    centered = values - mean
    variance = jnp.mean(centered * centered, axis=-1, keepdims=True)
    return centered * lax.rsqrt(variance + LN_EPS) * scale


def attend_one(operands):
    queries, keys, values = operands
    scores = jnp.einsum('nhd,mhd->hnm', queries.astype(jnp.float32), keys.astype(jnp.float32)) * HEAD_DIM ** -0.5
    attn_probs = jax.nn.softmax(scores, axis=-1).astype(jnp.bfloat16)
    attended = jnp.einsum('hnm,mhd->nhd', attn_probs.astype(jnp.float32), values.astype(jnp.float32))
    return attended.astype(jnp.bfloat16)


def reference(x, ln_scale, qn_scale, kn_scale, w_qkv, w_up, b_up, w_o, w_down, b_out):
    tokens = BATCH * PATCHES
    qkv_width = HEADS * HEAD_DIM
    x_flat = x.reshape(tokens, MODEL_DIM).astype(jnp.float32)
    normed = layer_norm(x_flat, ln_scale).astype(jnp.bfloat16)
    proj_qkv = jnp.dot(normed, w_qkv.reshape(MODEL_DIM, 3 * qkv_width), preferred_element_type=jnp.float32).astype(jnp.bfloat16)
    proj_qkv = proj_qkv.reshape(BATCH, PATCHES, 3, HEADS, HEAD_DIM)
    queries = layer_norm(proj_qkv[:, :, 0].astype(jnp.float32), qn_scale).astype(jnp.bfloat16)
    keys = layer_norm(proj_qkv[:, :, 1].astype(jnp.float32), kn_scale).astype(jnp.bfloat16)
    attended = lax.map(attend_one, (queries, keys, proj_qkv[:, :, 2]))
    up_in = jnp.dot(normed, w_up, preferred_element_type=jnp.float32).astype(jnp.bfloat16)
    hidden = jax.nn.gelu(up_in.astype(jnp.float32) + b_up, approximate=False).astype(jnp.bfloat16)
    mixed_sum = jnp.dot(attended.reshape(tokens, qkv_width), w_o, preferred_element_type=jnp.float32) + jnp.dot(hidden, w_down, preferred_element_type=jnp.float32)
    result = x_flat + mixed_sum + b_out
    return result.astype(jnp.bfloat16).reshape(BATCH, PATCHES, MODEL_DIM)
```

```python
import functools

import jax
import jax.numpy as jnp
from jax import lax
from jax.experimental import pallas as pl
from jax.experimental.pallas import tpu as pltpu
from jax.sharding import PartitionSpec as P

LN_EPS = 1e-6
BF = jnp.bfloat16
F32 = jnp.float32
ONE = pl.Buffered(1)
ROWS = 512
SUB = 256

PERM_Y = ((0, 1), (1, 0))
PERM_X = ((0, 2), (2, 0), (1, 3), (3, 1))
PERM_C = ((0, 1), (1, 0), (2, 3), (3, 2))


def params(n=1):
    return pltpu.CompilerParams(dimension_semantics=("arbitrary",) * n, vmem_limit_bytes=61 * 2**20)


def mm(a, b):
    return jnp.dot(a, b, preferred_element_type=F32)


def gelu(v):
    return 0.5 * v * (1.0 + lax.erf(v * 0.7071067811865476))


def up_proj(info, u_own, u_oth, weights, biases, n_rows):
    width = weights[0].shape[1]
    dim = u_own.shape[1]

    def body(info_ref, uo, ur, wao, wbo, was, wbs, *rest):
        if biases is None:
            zo, zs = rest
            bo = bs = None
        else:
            bo, bs, zo, zs = rest

        def step(r, carry):
            rows = pl.ds(pl.multiple_of(r * SUB, SUB), SUB)
            a, b = uo[rows, :], ur[rows, :]
            for wa, wb, bias, z in ((wao, wbo, bo, zo), (was, wbs, bs, zs)):
                acc = mm(a, wa[...]) + mm(b, wb[...])
                if bias is not None:
                    acc = gelu(acc.astype(BF).astype(F32) + bias[...])
                z[rows, :] = acc.astype(BF)
            return carry

        lax.fori_loop(0, ROWS // SUB, step, 0)

    w_spec = pl.BlockSpec((dim, width), lambda m, s: (0, 0), pipeline_mode=ONE)
    blocks = n_rows // ROWS
    in_specs = [
        pl.BlockSpec((ROWS, dim), lambda m, s: ((m + s[0] * (blocks // 2)) % blocks, 0)),
        pl.BlockSpec((ROWS, dim), lambda m, s: (m, 0)),
    ] + [w_spec] * 4
    args = [u_own, u_oth, *weights]
    if biases is not None:
        in_specs += [pl.BlockSpec((1, width), lambda m, s: (0, 0))] * 2
        args += list(biases)
    o_spec = pl.BlockSpec((ROWS, width), lambda m, s: (m, 0))
    return pl.pallas_call(
        body,
        grid_spec=pltpu.PrefetchScalarGridSpec(
            num_scalar_prefetch=1, grid=(blocks,), in_specs=in_specs, out_specs=[o_spec] * 2
        ),
        out_shape=[jax.ShapeDtypeStruct((n_rows, width), BF)] * 2,
        compiler_params=params(),
        cost_estimate=pl.CostEstimate(
            flops=2 * 2 * n_rows * 2 * dim * width, bytes_accessed=4 * n_rows * dim, transcendentals=0
        ),
    )(info, *args)


def attend(z_own, z_sib, qs, ks, n_rows, patches, head_dim):
    width = z_own.shape[1] // 3
    heads = width // head_dim

    def norm(v, scale):
        v = v.astype(F32)
        centered = v - jnp.mean(v, axis=-1, keepdims=True)
        var = jnp.mean(centered * centered, axis=-1, keepdims=True)
        return (centered * lax.rsqrt(var + LN_EPS) * scale).astype(BF)

    def body(zo, zs, qs_ref, ks_ref, oo, os):
        for z, o in ((zo, oo), (zs, os)):
            for h in range(heads):
                cols = slice(h * head_dim, (h + 1) * head_dim)
                q = norm(z[:, h * head_dim : (h + 1) * head_dim], qs_ref[...])
                k = norm(z[:, width + h * head_dim : width + (h + 1) * head_dim], ks_ref[...])
                v = z[:, 2 * width + h * head_dim : 2 * width + (h + 1) * head_dim]
                st = lax.dot_general(k, q, (((1,), (1,)), ((), ())), preferred_element_type=F32)
                st = st * head_dim**-0.5
                e = jnp.exp(st - jnp.max(st, axis=0, keepdims=True))
                p = (e / jnp.sum(e, axis=0, keepdims=True)).astype(BF)
                o[:, cols] = lax.dot_general(
                    p, v, (((0,), (0,)), ((), ())), preferred_element_type=F32
                ).astype(BF)

    z_spec = pl.BlockSpec((patches, 3 * width), lambda m: (m, 0))
    s_spec = pl.BlockSpec((1, head_dim), lambda m: (0, 0))
    o_spec = pl.BlockSpec((patches, width), lambda m: (m, 0))
    return pl.pallas_call(
        body,
        grid=(n_rows // patches,),
        in_specs=[z_spec, z_spec, s_spec, s_spec],
        out_specs=[o_spec] * 2,
        out_shape=[jax.ShapeDtypeStruct((n_rows, width), BF)] * 2,
        compiler_params=params(),
        cost_estimate=pl.CostEstimate(
            flops=8 * 2 * n_rows * patches * 2 * width, bytes_accessed=16 * n_rows * width, transcendentals=0
        ),
    )(z_own, z_sib, qs, ks)


def down_proj(info, h_own, h_sib, w_o, w_down, wo_sib, wd_sib, wr_own, wr_sib, q, width):
    n_rows = h_own[0].shape[0]
    k_o = wo_sib.shape[0]
    k_d = wd_sib.shape[0]
    blocks = n_rows // ROWS
    half = blocks // 2
    sizes = [h.shape[1] for h in h_own]
    n_h = len(sizes)

    def body(info_ref, *refs):
        ho, hs = refs[:n_h], refs[n_h : 2 * n_h]
        wlo, wld, wso, wsd, wro, wrs, lk, rk, sd = refs[2 * n_h :]

        def rows_of(r):
            rows = pl.ds(pl.multiple_of(r * SUB, SUB), SUB)
            left = right = None
            for hh, (a, b), w in ((ho, (wlo, wld), wro), (hs, (wso, wsd), wrs)):
                at = 0
                for ref, size in zip(hh, sizes):
                    lhs = ref[rows, :]
                    lw = a[at : at + size, :] if at < k_o else b[at - k_o : at - k_o + size, :]
                    pl_, pr_ = mm(lhs, lw), mm(lhs, w[at : at + size, :])
                    left = pl_ if left is None else left + pl_
                    right = pr_ if right is None else right + pr_
                    at += size
            return rows, left.astype(BF), right.astype(BF)

        def step(r, carry):
            rows, left, right = rows_of(r)

            @pl.when(pl.program_id(0) < half)
            def _():
                sd[0, rows, :] = left
                sd[1, rows, :] = right

            @pl.when(pl.program_id(0) >= half)
            def _():
                lk[rows, :] = left
                rk[rows, :] = right

            return carry

        lax.fori_loop(0, ROWS // SUB, step, 0)

    h_specs = [pl.BlockSpec((ROWS, s), lambda m, i: ((m + half) % blocks, 0)) for s in sizes]
    keep = pl.BlockSpec((ROWS, width), lambda m, i: (jnp.maximum(m - half, 0), 0))
    in_specs = h_specs + h_specs + [
        pl.BlockSpec((k_o, width), lambda m, i: (i[1], q), pipeline_mode=ONE),
        pl.BlockSpec((k_d, width), lambda m, i: (i[1], q), pipeline_mode=ONE),
        pl.BlockSpec((k_o, width), lambda m, i: (0, q), pipeline_mode=ONE),
        pl.BlockSpec((k_d, width), lambda m, i: (0, q), pipeline_mode=ONE),
        pl.BlockSpec((k_o + k_d, width), lambda m, i: (0, 0), pipeline_mode=ONE),
        pl.BlockSpec((k_o + k_d, width), lambda m, i: (0, 0), pipeline_mode=ONE),
    ]
    return pl.pallas_call(
        body,
        grid_spec=pltpu.PrefetchScalarGridSpec(
            num_scalar_prefetch=1,
            grid=(blocks,),
            in_specs=in_specs,
            out_specs=[
                keep,
                keep,
                pl.BlockSpec((2, ROWS, width), lambda m, i: (0, jnp.minimum(m, half - 1), 0)),
            ],
        ),
        out_shape=[
            jax.ShapeDtypeStruct((n_rows // 2, width), BF),
            jax.ShapeDtypeStruct((n_rows // 2, width), BF),
            jax.ShapeDtypeStruct((2, n_rows // 2, width), BF),
        ],
        compiler_params=params(),
        cost_estimate=pl.CostEstimate(
            flops=2 * n_rows * 2 * (k_o + k_d) * 2 * width, bytes_accessed=4 * n_rows * (k_o + k_d), transcendentals=0
        ),
    )(info, *h_own, *h_sib, w_o, w_down, wo_sib, wd_sib, wr_own, wr_sib)


def finish(info, out, x_flat, b_out, l_keep, s_recv, r_recv, q, width):
    n = l_keep.shape[0]

    def body(info_ref, *refs):
        if out is not None:
            refs = refs[1:]
        x_ref, b_ref, l_ref, s_ref, r_ref, o_ref, f_ref = refs
        total = l_ref[...].astype(F32) + s_ref[0].astype(F32) + r_ref[...].astype(F32)
        total = (x_ref[...].astype(F32) + total + b_ref[...]).astype(BF)
        o_ref[...] = total
        f_ref[...] = total

    blocks = n // ROWS
    place = pl.BlockSpec((ROWS, width), lambda m, i: (blocks * i[2] + m, q))
    flat = pl.BlockSpec((ROWS, width), lambda m, i: (m, 0))
    in_specs = [
        place,
        pl.BlockSpec((1, width), lambda m, i: (0, q)),
        flat,
        pl.BlockSpec((1, ROWS, width), lambda m, i: (0, m, 0)),
        flat,
    ]
    args = [x_flat, b_out, l_keep, s_recv, r_recv]
    alias = {}
    if out is not None:
        in_specs = [pl.BlockSpec(memory_space=pl.ANY)] + in_specs
        args = [out] + args
        alias = {1: 0}
    return pl.pallas_call(
        body,
        grid_spec=pltpu.PrefetchScalarGridSpec(
            num_scalar_prefetch=1, grid=(blocks,), in_specs=in_specs, out_specs=[place, flat]
        ),
        out_shape=[
            jax.ShapeDtypeStruct(x_flat.shape, BF),
            jax.ShapeDtypeStruct((n, width), BF),
        ],
        input_output_aliases=alias,
        compiler_params=params(),
        cost_estimate=pl.CostEstimate(flops=2**22, bytes_accessed=10 * n * width, transcendentals=0),
    )(info, *args)


def put(info, out, piece, slot, q, width):
    n = piece.shape[0]
    blocks = n // 1024

    def body(info_ref, out_ref, p_ref, o_ref):
        o_ref[...] = p_ref[...]

    return pl.pallas_call(
        body,
        grid_spec=pltpu.PrefetchScalarGridSpec(
            num_scalar_prefetch=1,
            grid=(blocks,),
            in_specs=[
                pl.BlockSpec(memory_space=pl.ANY),
                pl.BlockSpec((1024, width), lambda m, i: (m, 0)),
            ],
            out_specs=pl.BlockSpec((1024, width), lambda m, i: (blocks * i[slot] + m, q)),
        ),
        out_shape=jax.ShapeDtypeStruct(out.shape, BF),
        input_output_aliases={1: 0},
        compiler_params=params(),
        cost_estimate=pl.CostEstimate(flops=2**22, bytes_accessed=4 * n * width, transcendentals=0),
    )(info, out, piece)


def solution(mesh):
    def layer(x_blk, ln_scale, qn_scale, kn_scale, w_qkv, w_up, b_up, w_o, w_down, b_out):
        images, patches, dim = x_blk.shape
        head_dim = qn_scale.shape[0]
        y = lax.axis_index("m1")
        j = lax.axis_index("m2")
        x, c = j // 2, j % 2
        info = jnp.stack([x, y, 2 * c + x, 2 * c + 1 - x, 2 * (1 - c) + x, 2 * (1 - c) + 1 - x]).astype(jnp.int32)
        qs, ks = qn_scale.reshape(1, head_dim), kn_scale.reshape(1, head_dim)
        n_rows = images * patches // 2
        quarter = n_rows // 2
        x_flat = x_blk.reshape(images * patches, dim)

        q_half = w_qkv.shape[2] // 2
        u_half = w_up.shape[1] // 2
        k_o, k_d = w_o.shape[0] // 2, w_down.shape[0] // 2
        qkv_w = 256
        n_qkv = q_half // qkv_w
        up_w = [768, 768, 768, 512]
        up_at = [0, 768, 1536, 2304]

        def qkv_cols(side, i):
            cut = lax.dynamic_slice(w_qkv, (0, 0, side * q_half + i * qkv_w), (dim, 3, qkv_w))
            return jnp.concatenate([cut[:, 0], cut[:, 1], cut[:, 2]], axis=1)

        def up_cols(side, i):
            return lax.dynamic_slice(w_up, (0, side * u_half + up_at[i]), (dim, up_w[i]))

        n_up = len(up_w)
        cols = [functools.partial(qkv_cols, i=i) for i in range(n_qkv)]
        cols += [functools.partial(up_cols, i=i) for i in range(n_up)]

        w_b, w_bs, w_a, w_as = {}, {}, {}, {}

        def send_w(i):
            cut = cols[i](1 - y)
            w_b[i] = lax.ppermute(cut, "m1", PERM_Y)
            w_bs[i] = lax.ppermute(w_b[i], "m2", PERM_C)
            w_a[i] = cols[i](y)
            w_as[i] = lax.ppermute(w_a[i], "m2", PERM_C)

        send_w(0)

        x_half = lax.dynamic_slice(x_blk, (c * (images // 2), 0, 0), (images // 2, patches, dim)).astype(F32)
        mean_l = jnp.mean(x_half, axis=-1)
        m2_l = jnp.mean(jnp.square(x_half - mean_l[..., None]), axis=-1)
        stats = jnp.stack([mean_l, m2_l])
        stats_o = lax.ppermute(stats, "m1", PERM_Y)
        mean_o, m2_o = stats_o[0], stats_o[1]
        mean = 0.5 * (mean_l + mean_o)
        var = 0.5 * (m2_l + m2_o) + 0.25 * jnp.square(mean_l - mean_o)
        scale = lax.dynamic_slice_in_dim(ln_scale, y * dim, dim)
        u_own = ((x_half - mean[..., None]) * lax.rsqrt(var + LN_EPS)[..., None] * scale).astype(BF)
        u_own = u_own.reshape(n_rows, dim)
        n_piece = 2
        size = quarter // n_piece
        got_y, got_x = [], []
        for p in range(n_piece):
            cut = lax.dynamic_slice(u_own, (x * quarter + p * size, 0), (size, dim))
            got_y.append(lax.ppermute(cut, "m1", PERM_Y))
            got_x.append(lax.ppermute(got_y[-1], "m2", PERM_X))
        u_oth = jnp.concatenate(got_y + got_x, axis=0)

        for i in range(1, n_qkv + n_up):
            send_w(i)

        wo_own = lax.dynamic_slice(w_o, (y * k_o, 0), (k_o, dim))
        wd_own = lax.dynamic_slice(w_down, (y * k_d, 0), (k_d, dim))
        wo_sib = lax.ppermute(wo_own, "m2", PERM_C)
        wd_sib = lax.ppermute(wd_own, "m2", PERM_C)
        out_w = 512
        n_out = dim // out_w
        wr_own, wr_sib = [], []
        for q in range(n_out):
            cut = jnp.concatenate(
                [
                    lax.dynamic_slice(w_o, ((1 - y) * k_o, q * out_w), (k_o, out_w)),
                    lax.dynamic_slice(w_down, ((1 - y) * k_d, q * out_w), (k_d, out_w)),
                ],
                axis=0,
            )
            wr_own.append(lax.ppermute(cut, "m1", PERM_Y))
            wr_sib.append(lax.ppermute(wr_own[-1], "m2", PERM_C))

        h_own, h_sib = [], []
        for i in range(n_qkv):
            z_own, z_sib = up_proj(info, u_own, u_oth, (w_a[i], w_b[i], w_as[i], w_bs[i]), None, n_rows)
            o_own, o_sib = attend(z_own, z_sib, qs, ks, n_rows, patches, head_dim)
            h_own.append(o_own)
            h_sib.append(o_sib)
        b_own = lax.dynamic_slice_in_dim(b_up, y * u_half, u_half)
        b_sib = lax.ppermute(b_own, "m2", PERM_C)
        for t in range(n_up):
            i = n_qkv + t
            bias = tuple(b[up_at[t] : up_at[t] + up_w[t]].reshape(1, -1) for b in (b_own, b_sib))
            g_own, g_sib = up_proj(info, u_own, u_oth, (w_a[i], w_b[i], w_as[i], w_bs[i]), bias, n_rows)
            h_own.append(g_own)
            h_sib.append(g_sib)

        b_row = b_out.reshape(1, dim)
        out = None
        for q in range(n_out):
            l_keep, r_keep, s = down_proj(
                info, h_own, h_sib, w_o, w_down, wo_sib, wd_sib, wr_own[q], wr_sib[q], q, out_w
            )
            s_recv = lax.ppermute(s, "m2", PERM_X)
            r = (r_keep.astype(F32) + s_recv[1].astype(F32)).astype(BF)
            r_recv = lax.ppermute(r, "m1", PERM_Y)
            out, fin = finish(info, out, x_flat, b_row, l_keep, s_recv, r_recv, q, out_w)
            f_x = lax.ppermute(fin, "m2", PERM_X)
            f_c = lax.ppermute(fin, "m2", PERM_C)
            f_xc = lax.ppermute(f_x, "m2", PERM_C)
            out = put(info, out, f_x, 3, q, out_w)
            out = put(info, out, f_c, 4, q, out_w)
            out = put(info, out, f_xc, 5, q, out_w)
        return out.reshape(images, patches, dim)

    return jax.shard_map(
        layer,
        mesh=mesh,
        in_specs=(P("dp", None, "m1"), P(), P(), P(), P("m1", None, "m2"), P("m1", "m2"), P("m2"), P("m2", "m1"), P("m2", "m1"), P("m1")),
        out_specs=P("dp", None, "m1"),
        check_vma=False,
    )
```
